32 devices in a mesh: grp: 16 (over z, y, x), sub: 2 (over core).
Axes of the slice: x: 2, y: 2, z: 4, core: 2. Of those that a mesh axis runs over, the one named last changes fastest.
Arguments:
- potentials: bfloat16 [1024, 200, 200], P(('grp', 'sub')), may hold values from -6 to 6
- dimers: int32 [4096, 2], P(('grp', 'sub')), may hold values from 0 to 1023, as said below
- coupling: float32 [4096], P(('grp', 'sub')), may hold values from 0.3 to 1.5
- transform: bfloat16 [400, 400], replicated, may hold values from -0.3125 to 0.3125
Outputs:
- energies: float32 [4096, 400], P(('grp', 'sub'))
- checksum: float32 [1], replicated
The draws below stay inside these ranges and needn't reach their ends.
Inputs may be any that keep to these rules, and one draw needn't show every extreme that they name: `dimers`: each row names two different fragments. Rows d with d // 128 = o belong to owner o, and their second fragment f has f // 32 = o. Among the 128 first fragments of one owner's rows, at most 6 fall into the fragments of any one device (fragments f with f // 32 equal), and exactly 6 into some device's fragments.
All inputs are finite; a program needn't handle non-finite values.
Results may differ from the reference program's by a relative error of at most 0.0023.
Values may be sent and summed in bfloat16 or wider, within the bound.
No kernel may reach another device: no remote copies, remote signals or barrier semaphores. Data moves between devices by JAX's collectives and lax.ppermute only.
A program may use at most 192 MiB of HBM per device.

```python
import math
import jax
import jax.numpy as jnp
from jax import lax

B = 200
FRAG_DEV = 32
DIM_DEV = 128
OWNERS = 32
FRAGS = 1024
DIMERS = 4096
PAIR = 400
CAP = 6


def draw_dimers(key, part):

    def one_owner(owner, owner_key):
        key_full, key_rest, key_local, key_order, key_second = jax.random.split(owner_key, 5)
        full = jax.random.randint(key_full, (), 0, OWNERS)
        rest = jax.random.permutation(key_rest, OWNERS * CAP - CAP)
        rest = rest + CAP * (rest >= full * CAP).astype(jnp.int32)
        first = full * CAP + jnp.arange(CAP, dtype=jnp.int32)
        slots = jnp.concatenate([first, rest[:DIM_DEV - CAP]])
        source = slots // CAP
        local = jax.random.randint(key_local, (DIM_DEV,), 0, FRAG_DEV)
        order = jax.random.permutation(key_order, DIM_DEV)
        leading = (source * FRAG_DEV + local)[order]
        second_local = jax.random.randint(key_second, (DIM_DEV,), 0, FRAG_DEV)
        second = owner * FRAG_DEV + second_local
        moved = owner * FRAG_DEV + (second_local + 1) % FRAG_DEV
        second = jnp.where(leading == second, moved, second)
        return jnp.stack([leading, second], axis=1)
    owner_keys = jax.random.split(jax.random.fold_in(key, 7), OWNERS)
    owner_ids = jnp.arange(OWNERS, dtype=jnp.int32)
    return jax.vmap(one_owner)(owner_ids, owner_keys).reshape(DIMERS, 2).astype(jnp.int32)


def shard_levels(own_key, dims, shards, least, top_value):
    gain = 1.0
    for axis_at, shards_of in shards:
        steps = jax.random.uniform(jax.random.fold_in(jax.random.fold_in(own_key, 6), axis_at), (shards_of,), jnp.float32, least / len(shards), top_value / len(shards))
        gain = gain * jnp.repeat(jnp.exp(steps), dims[axis_at] // shards_of).reshape((-1,) + (1,) * (len(dims) - 1 - axis_at))
    return gain


def normal_values(rng, shape, scale, most, cuts=(), held_as=jnp.bfloat16):
    entries = scale * jax.random.normal(rng, shape, jnp.float32)
    if cuts:
        entries = entries * shard_levels(rng, shape, cuts, -0.22, 0.18)
    return jnp.clip(entries, -most, most).astype(held_as)


def setup_inputs(seed: int = 0) -> dict:
    seeds = jax.random.split(jax.random.key(seed), 5)
    return {
        "potentials": normal_values(seeds[0], (FRAGS, B, B), 1.0, 6.0, ((0, 32),)),
        "dimers": draw_dimers(jax.random.fold_in(seeds[4], 71), 0),
        "coupling": jnp.clip(jnp.exp(math.log(1.5) - 1.60943787 * jax.random.uniform(seeds[2], (DIMERS,), jnp.float32) ** shard_levels(seeds[2], (DIMERS,), ((0, 32),), -0.2, 0.2)), 0.3, 1.5),
        "transform": normal_values(seeds[3], (PAIR, PAIR), PAIR ** -0.5, 0.3125),
    }


def block_energies(left, right, scale, transform):
    upper = transform[:B].astype(jnp.float32)
    lower = transform[B:].astype(jnp.float32)
    left_f = left.astype(jnp.float32)
    right_f = right.astype(jnp.float32)
    cross = jnp.einsum('nab,nbc->nac', left_f, right_f)
    block = (cross * (scale[:, None, None] / jnp.sqrt(jnp.float32(B)))).astype(jnp.bfloat16).astype(jnp.float32)
    top = jnp.einsum('nab,bk->nak', left_f, upper) + jnp.einsum('nab,bk->nak', block, lower)
    bottom = jnp.einsum('nab,ak->nbk', block, upper) + jnp.einsum('nab,bk->nak', right_f, lower)
    return lax.optimization_barrier(jnp.sum(upper[None] * top, axis=1)) + lax.optimization_barrier(jnp.sum(lower[None] * bottom, axis=1))

def reference(potentials, dimers, coupling, transform):
    width = 8 if DIMERS % 8 == 0 else DIMERS
    pairs = dimers.reshape(DIMERS // width, width, 2)
    scales = coupling.reshape(DIMERS // width, width)

    def one_block(item):
        pair, scale = item
        left = jnp.take(potentials, pair[:, 0], axis=0)
        right = jnp.take(potentials, pair[:, 1], axis=0)
        return block_energies(left, right, scale, transform)
    energies = lax.map(one_block, (pairs, scales)).reshape(DIMERS, 2 * B)
    weights = (jnp.arange(DIMERS).astype(jnp.float32) + 1.0) / DIMERS
    checksum = 2.0 / DIMERS * jnp.sum(weights * lax.optimization_barrier(jnp.mean(energies * energies, axis=1)))
    return (energies, checksum.reshape(1))
```

```python
import functools

import jax
import jax.numpy as jnp
from jax import lax
from jax.experimental import pallas as pl
from jax.experimental.pallas import tpu as pltpu
from jax.sharding import PartitionSpec as P


AXES = ("grp", "sub")
PLANES = 4
CHUNKS = 4
BATCH = 4
DEPTH = 3
LANES = 128
f32 = jnp.float32
bf16 = jnp.bfloat16


def up(value, step):
    return (value + step - 1) // step * step


def fold_sizes(n):
    top = 96
    low = n - top
    body = up(n, 16)
    return top, low, body, body + up(low, 16)


def pack_body(src, dst):
    count, n, _ = src.shape
    top, low, body, rows = fold_sizes(n)
    lane = lax.broadcasted_iota(jnp.int32, (8, LANES), 1) // 8

    @pl.loop(0, count)
    def _(i):
        main = src[i, :, :LANES]
        rest = src[i, :, LANES:n].astype(f32)
        rest = jnp.concatenate([rest, jnp.zeros((n, 2 * LANES - n), f32)], axis=1)
        wide = lax.broadcasted_iota(jnp.int32, (low, LANES), 1)
        under = rest[top:]
        over = jnp.concatenate([pltpu.roll(rest[:top], 64, 1), jnp.zeros((low - top, LANES), f32)], axis=0)
        half = jnp.where(wide < 64, under, over)
        tails = [jnp.zeros((8, LANES), f32), jnp.zeros((8, LANES), f32)]
        for g in range(n // 8):
            part = pltpu.roll(rest[8 * g:8 * g + 8], (8 * (g % 16) - 64) % LANES, 1)
            tails[g // 16] = jnp.where(lane == g % 16, part, tails[g // 16])
        dst[i, :body, :] = jnp.concatenate([main.astype(f32), tails[0]], axis=0).astype(bf16)
        dst[i, body:, :] = jnp.concatenate([half, tails[1]], axis=0).astype(bf16)


def pack(potentials):
    count, n, _ = potentials.shape
    rows = fold_sizes(n)[3]
    return pl.pallas_call(
        pack_body,
        out_shape=jax.ShapeDtypeStruct((count, rows, LANES), bf16),
        name="pack",
    )(potentials)


def unpack(ref, n):
    top, low, body, rows = fold_sizes(n)
    main = ref[:body, :]
    fold = ref[body:, :]
    turned = pltpu.roll(fold[:top].astype(f32), 64, 1)
    left = jnp.concatenate([turned, fold.astype(f32)], axis=0)[:body]
    tails = [ref[body - 16:body, :].astype(f32)[8:], ref[rows - 16:rows, :].astype(f32)[8:]]
    parts = []
    for g in range(body // 8):
        shift = (64 - 8 * (g % 16)) % LANES
        tail = tails[min(g // 16, 1)]
        parts.append(pltpu.roll(tail, shift, 1) if shift else tail)
    right = jnp.concatenate(parts, axis=0)
    lane = lax.broadcasted_iota(jnp.int32, (body, LANES), 1)
    rest = jnp.where(lane < 64, left, right).astype(bf16)
    return main, rest


def meeting_plane(a, b):
    lo, hi = jnp.minimum(a, b), jnp.maximum(a, b)
    return jnp.where((lo == 2) & (hi == 3), 2, hi)


def return_step(at, owner):
    key = at * 4 + owner
    return jnp.where(key == 8, 2, jnp.where((key == 9) | (key == 12), 1, 0))


RETURNS = (((1, 0), (2, 3), (3, 1)), ((2, 1), (3, 0)), ((2, 0),))


class Layout:
    def __init__(self, owners, frag_dev, count):
        self.cols = owners // PLANES
        self.cap = max(2, (4 * count + 3 * owners - 1) // (3 * owners))
        self.own = up(self.cap * self.cols, 8)
        self.side = up(3 * self.cap, 8)
        self.z_at = self.own + self.cols * self.side
        self.rows = self.z_at + 3 * self.own
        self.jobs = up(self.rows, BATCH)
        self.frag_dev = frag_dev
        self.count = count


def meta_body(lay, me_ref, dimers, rec, out_row, cnt):
    me = me_ref[0]
    z, col = me // lay.cols, me % lay.cols

    @pl.loop(0, lay.cols + 4)
    def _(i):
        cnt[i] = 0

    @pl.loop(0, lay.count)
    def _(d):
        first = dimers[2 * d]
        second = dimers[2 * d + 1]
        holder = first // lay.frag_dev
        zh, ch = holder // lay.cols, holder % lay.cols
        zm = meeting_plane(zh, z)
        same = zh == z
        side = (zm == z) & jnp.logical_not(same)
        step = return_step(zm, z)
        group = jnp.where(same, 0, jnp.where(side, 4 + ch, 1 + step))
        rank = cnt[group]
        cnt[group] = rank + 1
        z_row = lay.z_at + step * lay.own + rank
        at = jnp.where(same, rank, jnp.where(side, lay.own + col * lay.side + rank, z_row))
        back = jnp.where(same, rank, jnp.where(side, lay.own + ch * lay.side + rank, z_row))
        device = jnp.where(same, me, zm * lay.cols + jnp.where(side, ch, col))
        rec[d] = first
        rec[lay.count + d] = second
        rec[2 * lay.count + d] = at
        rec[3 * lay.count + d] = device
        out_row[d] = back


def stage_of(kind, chunk):
    last = CHUNKS - 1
    if kind == "L":
        return 0
    if kind == "C":
        return 2 if chunk == last else (1 if chunk == last - 1 else 0)
    return 1 if chunk == last else 0


STAGES = 3
KINDS = ("A", "B", "C", "L")


def sources(stage):
    return [(k, c) for k in KINDS for c in range(CHUNKS) if stage_of(k, c) == stage]


def plan_body(lay, me_ref, rec, base, jobs, counts):
    me = me_ref[0]
    z, col = me // lay.cols, me % lay.cols
    size = lay.frag_dev // CHUNKS
    half = lay.frag_dev // 2
    for s in range(STAGES):
        counts[s] = 0

    def plane_row(frag):
        c = (frag // lay.frag_dev) % lay.cols
        local = frag % lay.frag_dev
        return base[2 * c + local // half] + local % half

    def scan(owner):
        start = owner * 4 * lay.count

        @pl.loop(0, lay.count)
        def _(d):
            @pl.when(rec[start + 3 * lay.count + d] == me)
            def _():
                first = rec[start + d]
                second = rec[start + lay.count + d]
                zh = first // lay.frag_dev // lay.cols
                zo = owner // lay.cols
                same = zh == zo
                first_moves = same | (zh != z)
                mover = jnp.where(first_moves, first, second)
                other = jnp.where(first_moves, second, first)
                zv = jnp.where(first_moves, zh, zo)
                local = mover % lay.frag_dev
                chunk = local // size
                kind = jnp.where(zv == 3, 3, z - zv - 1)
                stage = jnp.int32(0)
                number = jnp.int32(0)
                for s in range(STAGES):
                    for n, (k, c) in enumerate(sources(s)):
                        hit = (kind == KINDS.index(k)) & (chunk == c)
                        stage = jnp.where(hit, s, stage)
                        number = jnp.where(hit, n + 1, number)
                stage = jnp.where(same, 0, stage)
                number = jnp.where(same, 0, number)
                z_row = jnp.where(same, plane_row(mover), local % size)
                slot = counts[stage]
                counts[stage] = slot + 1
                at = stage * 5 * lay.jobs + slot
                jobs[at] = plane_row(other)
                jobs[at + lay.jobs] = number
                jobs[at + 2 * lay.jobs] = z_row
                jobs[at + 3 * lay.jobs] = rec[start + 2 * lay.count + d] * 2 + jnp.where(first_moves, 1, 0)
                jobs[at + 4 * lay.jobs] = owner * lay.count + d

    @pl.loop(0, lay.cols)
    def _(c):
        scan(z * lay.cols + c)

    @pl.loop(0, PLANES)
    def _(p):
        @pl.when(p != z)
        def _():
            scan(p * lay.cols + col)


def energy_body(lay, n, stage, early_rows, z_count, jobs, counts, scales, upper, lower, upper_f, lower_f, prev, *rest):
    planes = rest[:2]
    zs = rest[2:2 + z_count]
    out, buf, sems = rest[2 + z_count:]
    body = fold_sizes(n)[2]
    total = counts[stage]
    offset = stage * 5 * lay.jobs
    batches = (total + BATCH - 1) // BATCH
    if prev is not None:
        out[...] = prev[...]

    def start(job, slot):
        j = jnp.minimum(job, total - 1)
        row = jobs[offset + j]
        number = jobs[offset + lay.jobs + j]
        z_row = jobs[offset + 2 * lay.jobs + j]
        code = jobs[offset + 3 * lay.jobs + j]
        place = code % 2

        def plane_copy(r, which, sem):
            @pl.when(r < early_rows)
            def _():
                pltpu.make_async_copy(planes[0].at[r], buf.at[slot, which], sems.at[slot, sem]).start()

            @pl.when(r >= early_rows)
            def _():
                pltpu.make_async_copy(planes[1].at[r - early_rows], buf.at[slot, which], sems.at[slot, sem]).start()

        plane_copy(row, place, 0)
        if stage == 0:
            @pl.when(number == 0)
            def _():
                plane_copy(z_row, 1 - place, 1)

        for i, z_ref in enumerate(zs):
            @pl.when(number == i + 1)
            def _(z_ref=z_ref):
                pltpu.make_async_copy(z_ref.at[z_row], buf.at[slot, 1 - place], sems.at[slot, 1]).start()

    def batch_start(b):
        for k in range(BATCH):
            start(b * BATCH + k, (b % DEPTH) * BATCH + k)

    @pl.when(total > 0)
    def _():
        for b in range(DEPTH - 1):
            @pl.when(b < batches)
            def _(b=b):
                batch_start(b)

        @pl.loop(0, batches)
        def _(b):
            @pl.when(b + DEPTH - 1 < batches)
            def _():
                batch_start(b + DEPTH - 1)

            group = (b % DEPTH) * BATCH
            for k in range(BATCH):
                for s in range(2):
                    pltpu.make_async_copy(planes[0].at[0], buf.at[group + k, s], sems.at[group + k, s]).wait()
            for k in range(BATCH):
                j = jnp.minimum(b * BATCH + k, total - 1)
                row = jobs[offset + 3 * lay.jobs + j] // 2
                scale = scales[jobs[offset + 4 * lay.jobs + j]]
                second = jnp.concatenate(unpack(buf.at[group + k, 1], n), axis=1)
                first = jnp.concatenate(unpack(buf.at[group + k, 0], n), axis=1)
                right = jnp.dot(second, lower[...], preferred_element_type=f32)[:n]
                left = lax.dot_general(first, upper[...], (((0,), (0,)), ((), ())), preferred_element_type=f32)[:n]
                terms = left * (upper_f[...] + scale * right) + right * lower_f[...]
                out[pl.ds(row, 1), :] = jnp.sum(terms, axis=0, keepdims=True)


def energies_of(lay, n, stage, jobs, counts, scales, tables, prev, planes, zs):
    width = tables[0].shape[1]
    smem = pl.BlockSpec(memory_space=pltpu.SMEM)
    vmem = pl.BlockSpec(memory_space=pltpu.VMEM)
    hbm = pl.BlockSpec(memory_space=pl.ANY)
    early = planes[0].shape[0]
    rows = fold_sizes(n)[3]
    has_prev = prev is not None
    body = functools.partial(energy_body, lay, n, stage, early, len(zs))
    if not has_prev:
        full = body

        def body(j, c, s, u, l, uf, lf, *rest):
            full(j, c, s, u, l, uf, lf, None, *rest)

    work = lay.count
    return pl.pallas_call(
        body,
        out_shape=jax.ShapeDtypeStruct((lay.rows, width), f32),
        in_specs=[smem] * 3 + [vmem] * 4 + [vmem] * has_prev + [hbm] * (2 + len(zs)),
        out_specs=vmem,
        scratch_shapes=[
            pltpu.VMEM((DEPTH * BATCH, 2, rows, LANES), bf16),
            pltpu.SemaphoreType.DMA((DEPTH * BATCH, 2)),
        ],
        input_output_aliases={7: 0} if has_prev else {},
        cost_estimate=pl.CostEstimate(
            flops=work * 4 * n * n * width, bytes_accessed=work * 2 * rows * LANES * 2, transcendentals=0),
        name="energies" + str(stage),
    )(jobs, counts, scales, *tables, *([prev] if has_prev else []), *planes, *zs)


def local(potentials, dimers, coupling, transform):
    frag_dev, n, _ = potentials.shape
    count = dimers.shape[0]
    chips = lax.axis_size("grp")
    cores = lax.axis_size("sub")
    owners = chips * cores
    lay = Layout(owners, frag_dev, count)
    per = chips // PLANES
    nx = max(d for d in range(1, per + 1) if per % d == 0 and d * d <= per)
    ny = per // nx
    me = lax.axis_index(AXES)
    barrier = lax.optimization_barrier

    def index(z, y, x, c):
        return ((z * ny + y) * nx + x) * cores + c

    every = [(z, y, x, c) for z in range(PLANES) for y in range(ny) for x in range(nx) for c in range(cores)]

    def send(value, pairs):
        return lax.ppermute(value, AXES, pairs)

    def along_z(value, hops):
        hop = dict(hops)
        return send(value, [(index(z, y, x, c), index(hop[z], y, x, c)) for z, y, x, c in every if z in hop])

    def shift(value, dy, dx, dc):
        return send(value, [
            (index(z, y, x, c), index(z, (y + dy) % ny, (x + dx) % nx, (c + dc) % cores)) for z, y, x, c in every])

    def after(value, other):
        return barrier((value, other[:1, :8, :]))[0]

    half = frag_dev // 2
    size = frag_dev // CHUNKS
    halves = [pack(potentials[:half]), pack(potentials[half:])]
    per_half = half // size
    chunks = [halves[c // per_half][(c % per_half) * size:(c % per_half + 1) * size] for c in range(CHUNKS)]
    moved = {k: [] for k in KINDS}
    for c in range(CHUNKS):
        own = chunks[c]
        if c >= 2:
            own = after(own, moved["B"][c - 2])
        moved["A"].append(along_z(own, ((0, 1), (1, 2))))
        moved["B"].append(along_z(moved["A"][c], ((1, 2), (2, 3))))
        moved["C"].append(along_z(moved["B"][c], ((2, 3),)))
    for c in range(CHUNKS):
        moved["L"].append(along_z(chunks[c], ((3, 2),)))

    pieces = {}
    for h in range(2):
        own = halves[h]
        late = after(own, moved["A"][1])
        for dx in range(nx):
            for dy in range(ny):
                if h == 0:
                    if dy == 0:
                        value = shift(own, 0, dx, 0) if dx else own
                    else:
                        value = shift(after(pieces[0, 0, dx, 0] if dx else late, moved["A"][1]), dy, 0, 0)
                else:
                    continue
                pieces[0, h, dx, dy] = value
        if h == 1:
            for dy in range(ny):
                for dx in range(nx):
                    if dx == 0:
                        value = shift(own, dy, 0, 0) if dy else own
                    else:
                        value = shift(after(pieces[0, 1, 0, dy] if dy else late, moved["A"][1]), 0, dx, 0)
                    pieces[0, h, dx, dy] = value
    for dc in range(1, cores):
        for h in range(2):
            for dx in range(nx):
                for dy in range(ny):
                    pieces[dc, h, dx, dy] = shift(pieces[0, h, dx, dy], 0, 0, dc)
    order = [k for k in pieces if not (k[2] and k[3])] + [k for k in pieces if k[2] and k[3]]
    early_count = sum(1 for k in order if not (k[2] and k[3]))
    planes = (
        jnp.concatenate([pieces[k] for k in order[:early_count]], axis=0),
        jnp.concatenate([pieces[k] for k in order[early_count:]], axis=0),
    )
    where = jnp.zeros((cores, 2, nx, ny), jnp.int32)
    place = {k: i * half for i, k in enumerate(order)}
    flat = jnp.array([place[dc, h, dx, dy] for dc in range(cores) for h in range(2) for dx in range(nx)
                      for dy in range(ny)], jnp.int32)
    col = me % lay.cols
    my_c, my_x, my_y = col % cores, col // cores % nx, col // cores // nx
    cols = jnp.arange(lay.cols, dtype=jnp.int32)
    dc = (my_c - cols % cores) % cores
    dx = (my_x - cols // cores % nx) % nx
    dy = (my_y - cols // cores // nx) % ny
    spot = jnp.stack([((dc * 2 + h) * nx + dx) * ny + dy for h in range(2)], axis=1).reshape(-1)
    base = jnp.sum(jnp.where(spot[:, None] == jnp.arange(flat.shape[0])[None, :], flat[None, :], 0), axis=1)

    smem = pl.BlockSpec(memory_space=pltpu.SMEM)
    me_arr = me.reshape(1).astype(jnp.int32)
    rec, back = pl.pallas_call(
        functools.partial(meta_body, lay),
        out_shape=(jax.ShapeDtypeStruct((4 * count,), jnp.int32), jax.ShapeDtypeStruct((count,), jnp.int32)),
        in_specs=[smem, smem],
        out_specs=(smem, smem),
        scratch_shapes=[pltpu.SMEM((lay.cols + 4,), jnp.int32)],
        name="meta",
    )(me_arr, dimers.reshape(-1))
    scale = coupling * (2.0 / jnp.sqrt(f32(n)))
    shared = lax.all_gather(jnp.concatenate([rec.astype(f32), scale]), AXES, axis=0, tiled=False)
    everyone = shared[:, :4 * count].astype(jnp.int32).reshape(-1)
    scales = shared[:, 4 * count:].reshape(-1)
    jobs, counts = pl.pallas_call(
        functools.partial(plan_body, lay),
        out_shape=(jax.ShapeDtypeStruct((STAGES * 5 * lay.jobs,), jnp.int32),
                   jax.ShapeDtypeStruct((STAGES,), jnp.int32)),
        in_specs=[smem] * 3,
        out_specs=(smem, smem),
        name="plan",
    )(me_arr, everyone, base)

    body = fold_sizes(n)[2]
    width = up(2 * n, LANES)
    pad = width - transform.shape[1]
    upper = jnp.pad(transform[:n], ((0, body - n), (0, pad)))
    lower = jnp.pad(transform[n:], ((0, 2 * LANES - n), (0, pad)))
    tables = (upper, lower, upper[:n].astype(f32), lower[:n].astype(f32))
    result = None
    for s in range(STAGES):
        zs = [moved[k][c] for k, c in sources(s)]
        result = energies_of(lay, n, s, jobs, counts, scales, tables, result, planes, zs)

    parts = [result[:lay.own]]
    side = result[lay.own:lay.z_at].reshape(lay.cols, lay.side, width)
    groups = [[p * lay.cols + c for c in range(lay.cols)] for p in range(PLANES)]
    got = lax.all_to_all(side, AXES, split_axis=0, concat_axis=0, axis_index_groups=groups, tiled=True)
    parts.append(got.reshape(lay.cols * lay.side, width))
    for i, hops in enumerate(RETURNS):
        at = lay.z_at + i * lay.own
        parts.append(along_z(result[at:at + lay.own], hops))
    energies = jnp.take(jnp.concatenate(parts, axis=0), back, axis=0)[:, :2 * n]
    total = count * owners
    position = me * count + jnp.arange(count, dtype=jnp.int32)
    weights = (position.astype(f32) + 1.0) / total
    partial_value = 2.0 / total * jnp.sum(weights * jnp.mean(energies * energies, axis=1))
    checksum = lax.psum(partial_value, AXES)
    return (energies, checksum.reshape(1))


def solution(mesh):
    in_specs = (P(AXES, None, None), P(AXES, None), P(AXES), P())
    out_specs = (P(AXES, None), P())
    return jax.shard_map(local, mesh=mesh, in_specs=in_specs, out_specs=out_specs, check_vma=False)
```
